32 devices in a mesh: groups: 2 (over y), mp: 2 (over x), expert: 4 (over z), dp: 2 (over core).
Axes of the slice: x: 2, y: 2, z: 4, core: 2. Of those that a mesh axis runs over, the one named last changes fastest.
Arguments:
- hidden_in: bfloat16 [1024, 4096], P(('groups', 'expert', 'dp'), 'mp'), parts along dimension 0, may hold values from -6 to 6
- norm_gain: bfloat16 [2, 4096], P(None, 'mp'), may hold values from 0.25 to 1.75
- expert_ids: int32 [2, 1024, 2], P(None, ('groups', 'expert', 'dp')), parts along dimension 1, may hold values from 0 to 3, all different within a row; in each aligned block of 64 rows (0 to 63, 64 to 127, ..., all dimensions but the last counted through in order) at most 64 rows name the same one
- gate_counts: int32 [2, 1024, 2], P(None, ('groups', 'expert', 'dp')), parts along dimension 1, may hold values from 8 to 15
- exit_layer: int32 [1024], P(('groups', 'expert', 'dp')), parts along dimension 0, may hold values from 1 to 2
- w_gate: bfloat16 [2, 4, 7168, 4096], P(None, 'expert', ('mp', 'dp')), may hold values from -0.09375 to 0.09375
- w_up: bfloat16 [2, 4, 7168, 4096], P(None, 'expert', ('mp', 'dp')), may hold values from -0.09375 to 0.09375
- w_down: bfloat16 [2, 4, 7168, 4096], P(None, 'expert', ('mp', 'dp')), may hold values from -0.0625 to 0.0625
Outputs:
- hidden_out: bfloat16 [1024, 4096], P(('groups', 'expert', 'dp'), 'mp'), parts along dimension 0
The draws below stay inside these ranges and needn't reach their ends.
There are 2 independent parts, one for each index of `groups`. The reference program is written for one: setup_inputs(seed, part) draws one part's arguments, and reference() takes and returns one part's arrays. A program takes and returns all parts, laid end to end along the dimension named above; an argument that names none is the same for every part. Nothing has to cross between parts.
Inputs may be any that keep to these rules, and one draw needn't show every extreme that they name: `expert_ids`: A token's two ids in a layer differ. In the rows of one device in one layer (aligned blocks of 64 rows, layer by layer) some expert may be named by all 64 rows.
All inputs are finite; a program needn't handle non-finite values.
Results may differ from the reference program's by a relative error of at most 0.014.
Values may be sent and summed in bfloat16 or wider, within the bound.
No kernel may reach another device: no remote copies, remote signals or barrier semaphores. Data moves between devices by JAX's collectives and lax.ppermute only.
A program may use at most 384 MiB of HBM per device.

```python
import math
import jax
import jax.numpy as jnp
import numpy as np
from jax import lax

D = 4096
FF = 7168
LAYERS = 2
TOK_DEV = 64
EXPERTS = 4
TOKENS = 512
N_MP = 2


def draw_exit_layer(key, part):
    own_key = jax.random.fold_in(key, 17)
    key_roll, key_early = jax.random.split(own_key)
    roll_value = jax.random.randint(key_roll, (TOKENS,), 0, 100)
    early_exit = jax.random.randint(key_early, (TOKENS,), 1, max(LAYERS, 2))
    exits = jnp.where(roll_value < 95, LAYERS, early_exit)
    position = jnp.arange(TOKENS)
    exits = jnp.where(position == 0, 1, jnp.where(position == 1, LAYERS, exits))
    return exits.astype(jnp.int32)


def place_ends(array, stream_key, least, largest):
    place = [jax.random.randint(jax.random.fold_in(stream_key, axis), (), 0, length) for axis, length in enumerate(array.shape)]
    main_axis = array.shape.index(max(array.shape))
    beside = place[:main_axis] + [(place[main_axis] + 1) % array.shape[main_axis]] + place[main_axis + 1:]
    return array.at[tuple(place)].set(least).at[tuple(beside)].set(largest)


def shard_levels(rng, dims, cuts, smallest, high):
    def one(dim, parts):
        steps = jax.random.uniform(jax.random.fold_in(jax.random.fold_in(rng, 6), dim), (parts,), jnp.float32, smallest / len(cuts), high / len(cuts))
        return jnp.repeat(jnp.exp(steps), dims[dim] // parts).reshape((-1,) + (1,) * (len(dims) - dim - 1))

    loudness = one(*cuts[0])
    for cut in cuts[1:]:
        loudness = loudness * one(*cut)
    return loudness


def routed_block(key, own, number, rows, amount, top, limit, skew):
    order = jax.random.permutation(key, amount)
    packed, ordinary = portions_of(amount, rows * top, limit, skew, True), portions_of(amount, rows * top, limit, skew, False)
    places = jnp.arange(amount)

    def named(sizes, turn):
        used = int((sizes > 0).sum())
        fixed = max(1, used // 4)
        shifted = fixed + (places - fixed + turn * (used - fixed)) % max(1, amount - fixed)
        return jnp.zeros((amount,), jnp.int32).at[order[jnp.where(places < fixed, places, shifted)]].set(jnp.asarray(sizes, jnp.int32))

    sizes = jnp.where(number % 4 == 0, named(packed, number // 4), named(ordinary, number - number // 4 - 1))
    mixed = jax.random.permutation(jax.random.fold_in(own, 3), amount)
    source_of, taker = mixed[0:amount // 2 * 2:2], mixed[1:amount // 2 * 2:2]
    slack = jnp.minimum(sizes[source_of] - 1, limit - sizes[taker]) // 2
    slack = jnp.where((source_of == order[0]) | (taker == order[0]) | (sizes[taker] == 0), 0, jnp.maximum(slack, 0))
    shifted = jax.random.randint(jax.random.fold_in(own, 4), (amount // 2,), 0, 1 << 20) % (slack + 1)
    sizes = sizes.at[source_of].add(-shifted).at[taker].add(shifted)
    members = jnp.searchsorted(jnp.cumsum(sizes), jnp.arange(rows * top), side="right").astype(jnp.int32)
    table = members.reshape(top, rows).T
    table = table[jax.random.permutation(jax.random.fold_in(own, 1), rows)]
    turn = jax.random.randint(jax.random.fold_in(own, 2), (rows, 1), 0, top)
    return jnp.take_along_axis(table, (jnp.arange(top)[None, :] + turn) % top, axis=1)


def portions_of(count, total, reach, lean, full):
    portions = [(1 << 20) // math.isqrt(standing ** lean) + 1 for standing in range(1, count + 1)]
    largest = reach if full else min(reach, max(-(-total // count), total * portions[0] // sum(portions)))
    least = 1 if total - largest >= count - 1 else 0
    holding, surplus = [largest] + [least] * (count - 1), total - largest - least * (count - 1)
    while surplus > 0:
        free = [i for i in range(1, count) if holding[i] < largest] or [i for i in range(1, count) if holding[i] < reach]
        whole, left = sum([portions[i] for i in free]), surplus
        for i in free:
            more = min(reach - holding[i], max(1, left * portions[i] // whole), surplus)
            holding[i] = holding[i] + more
            surplus = surplus - more
    return np.array(holding)


def centred(key, shape, deviation, most, pieces=(), held_as=jnp.bfloat16):
    drawn = jax.random.normal(key, shape, jnp.float32) * deviation
    if len(pieces) > 0:
        drawn = shard_levels(key, shape, pieces, -0.22, 0.18) * drawn
    return jnp.clip(drawn, min=-most, max=most).astype(held_as)


def setup_inputs(seed: int = 0, part: int = 0) -> dict:
    key_of = jax.random.split(jax.random.key(seed), 9)
    own_keys = jax.random.split(jax.random.fold_in(key_of[8], part), 9)
    hidden_in = centred(own_keys[0], (TOKENS, D), 1.0, 6.0, ((0, 8), (1, 2)))
    norm_gain = jnp.clip(1.0 + 0.15 * jax.random.normal(key_of[1], (LAYERS, D), jnp.float32), 0.25, 1.75).astype(jnp.bfloat16)
    expert_ids_keys = jax.random.split(jax.random.fold_in(own_keys[2], 1), LAYERS * TOKENS // TOK_DEV)
    expert_ids_turns = jax.random.permutation(jax.random.fold_in(own_keys[2], 3), LAYERS * TOKENS // TOK_DEV)
    expert_ids = jax.vmap(lambda own, number: routed_block(jax.random.fold_in(own_keys[2], 2), own, number, TOK_DEV, EXPERTS, 2, TOK_DEV, 2))(expert_ids_keys, expert_ids_turns).reshape((LAYERS, TOKENS, 2))
    gate_counts = place_ends(jax.random.randint(own_keys[3], (LAYERS, TOKENS, 2), 8, 16), jax.random.fold_in(own_keys[3], 1), 8, 15).astype(jnp.int32)
    exit_layer = draw_exit_layer(jax.random.fold_in(jax.random.fold_in(key_of[8], part), 71), part)
    w_gate = centred(key_of[5], (LAYERS, EXPERTS, FF, D), D ** -0.5, 0.09375, ((1, 4), (2, 4)))
    w_up = centred(key_of[6], (LAYERS, EXPERTS, FF, D), D ** -0.5, 0.09375, ((1, 4), (2, 4)))
    w_down = centred(key_of[7], (LAYERS, EXPERTS, FF, D), FF ** -0.5, 0.0625, ((1, 4), (2, 4)))
    return {"hidden_in": hidden_in, "norm_gain": norm_gain, "expert_ids": expert_ids, "gate_counts": gate_counts, "exit_layer": exit_layer, "w_gate": w_gate, "w_up": w_up, "w_down": w_down}


norm_floor = 0.1

def expert_output(normed, gate_rows, up_rows, down_rows):
    contract = (((1,), (1,)), ((), ()))
    gate_val = lax.dot_general(normed, gate_rows, contract, preferred_element_type=jnp.float32)
    up_val = lax.dot_general(normed, up_rows, contract, preferred_element_type=jnp.float32)
    hidden = (jax.nn.silu(gate_val) * up_val).astype(jnp.bfloat16)
    block_len = FF // N_MP
    running = jnp.zeros((normed.shape[0], D), jnp.float32)
    for block_idx in range(N_MP):
        row_start = block_idx * block_len
        partial_value = jnp.dot(hidden[:, row_start:row_start + block_len], down_rows[row_start:row_start + block_len], preferred_element_type=jnp.float32)
        rounded = lax.optimization_barrier(partial_value.astype(jnp.bfloat16))
        running = running + rounded.astype(jnp.float32)
    return running.astype(jnp.bfloat16)

def reference(hidden_in, norm_gain, expert_ids, gate_counts, exit_layer, w_gate, w_up, w_down):
    current = hidden_in
    expert_range = jnp.arange(EXPERTS, dtype=jnp.int32)
    for layer_idx in range(LAYERS):
        current_f32 = current.astype(jnp.float32)
        sum_squares = lax.optimization_barrier(jnp.sum(current_f32 * current_f32, axis=1, keepdims=True))
        inv_rms = lax.rsqrt(sum_squares / D + norm_floor)
        normed = (current_f32 * inv_rms * norm_gain[layer_idx].astype(jnp.float32)[None, :]).astype(jnp.bfloat16)
        outputs = lax.map(lambda weights: expert_output(normed, weights[0], weights[1], weights[2]), (w_gate[layer_idx], w_up[layer_idx], w_down[layer_idx]))
        counts = gate_counts[layer_idx].astype(jnp.float32)
        gate_share = counts / lax.optimization_barrier(jnp.sum(counts, axis=1, keepdims=True))
        matched = expert_ids[layer_idx][:, :, None] == expert_range[None, None, :]
        weight_te = lax.optimization_barrier(jnp.sum(jnp.where(matched, gate_share[:, :, None], jnp.float32(0.0)), axis=1))
        active = (exit_layer > layer_idx).astype(jnp.float32)
        weight_te = weight_te * active[:, None]
        update = jnp.einsum('te,etd->td', weight_te, outputs.astype(jnp.float32), precision=lax.Precision.HIGHEST)
        current = (current_f32 + update).astype(jnp.bfloat16)
    return current
```

```python
import jax
import jax.numpy as jnp
from jax import lax
from jax.sharding import PartitionSpec as P

CHUNKS = 2
norm_floor = 0.1


def gather_rows(rows):
    rows = lax.all_gather(rows, "mp", axis=1, tiled=True)
    return lax.all_gather(rows, ("expert", "dp"), axis=0, tiled=True)


def scatter_rows(part):
    part = lax.psum_scatter(part, ("expert", "dp"), scatter_dimension=0, tiled=True)
    return lax.psum_scatter(part, "mp", scatter_dimension=1, tiled=True)


def layer(current, gain, weight, gate_rows, up_rows, down_rows):
    contract = (((1,), (1,)), ((), ()))
    whole_f32 = gather_rows(current).astype(jnp.float32)
    inv_rms = lax.rsqrt(jnp.sum(whole_f32 * whole_f32, axis=1) / whole_f32.shape[1] + norm_floor)
    normed = (whole_f32 * inv_rms[:, None] * gain[None, :]).astype(jnp.bfloat16)
    gate_val = lax.dot_general(normed, gate_rows, contract, preferred_element_type=jnp.float32)
    up_val = lax.dot_general(normed, up_rows, contract, preferred_element_type=jnp.float32)
    hidden = (jax.nn.silu(gate_val) * up_val).astype(jnp.bfloat16)
    part = jnp.dot(hidden, down_rows, preferred_element_type=jnp.float32)
    update = scatter_rows((part * weight[:, None]).astype(jnp.bfloat16))
    return (current.astype(jnp.float32) + update.astype(jnp.float32)).astype(jnp.bfloat16)


def body(hidden_in, norm_gain, expert_ids, gate_counts, exit_layer, w_gate, w_up, w_down):
    layers = norm_gain.shape[0]
    tok_rows = hidden_in.shape[0]
    experts = lax.axis_size("expert")
    counts = gate_counts.astype(jnp.float32)
    share = counts / jnp.sum(counts, axis=2, keepdims=True)
    active = exit_layer[None, :] > jnp.arange(layers, dtype=jnp.int32)[:, None]
    matched = expert_ids[:, :, :, None] == jnp.arange(experts, dtype=jnp.int32)
    matched = matched & active[:, :, None, None]
    weight = jnp.sum(jnp.where(matched, share[..., None], jnp.float32(0.0)), axis=2)
    weight = lax.all_gather(weight, ("expert", "dp"), axis=0)
    own = lax.axis_index("expert")
    weight = lax.dynamic_index_in_dim(weight, own, axis=3, keepdims=False)
    gain = lax.all_gather(norm_gain, "mp", axis=1, tiled=True).astype(jnp.float32)
    step = tok_rows // CHUNKS
    streams = [hidden_in[c * step:(c + 1) * step] for c in range(CHUNKS)]
    for l in range(layers):
        for c in range(CHUNKS):
            rows = weight[:, l, c * step:(c + 1) * step].reshape(-1)
            streams[c] = layer(
                streams[c], gain[l], rows, w_gate[l, 0], w_up[l, 0], w_down[l, 0]
            )
    return jnp.concatenate(streams, axis=0)


def solution(mesh):
    in_specs = (
        P(("groups", "expert", "dp"), "mp"),
        P(None, "mp"),
        P(None, ("groups", "expert", "dp"), None),
        P(None, ("groups", "expert", "dp"), None),
        P(("groups", "expert", "dp")),
        P(None, "expert", ("mp", "dp"), None),
        P(None, "expert", ("mp", "dp"), None),
        P(None, "expert", ("mp", "dp"), None),
    )
    out_specs = P(("groups", "expert", "dp"), "mp")
    return jax.shard_map(body, mesh=mesh, in_specs=in_specs, out_specs=out_specs, check_vma=False)
```
